128 devices in a mesh: gx: 8 (over y_lo, z), gy: 4 (over x), gz: 4 (over y_hi, core).
Axes of the slice: x: 4, y: 4 (y_hi: 2, y_lo: 2; y = y_hi * 2 + y_lo), z: 4, core: 2. Of those that a mesh axis runs over, the one named last changes fastest.
Arguments:
- snapshots: float32 [4, 4, 4096, 8192], P(None, 'gz', 'gx', 'gy'), may hold values from -6 to 6
- steps: int32 [4], replicated, may hold values from 0 to 3999
- mask: int32 [4, 64], replicated, may hold values 0 or 1
- probe: float32 [4096], replicated, may hold values from -6 to 6
Outputs:
- weights: bfloat16 [4, 4096, 8192], P(None, ('gx', 'gy'), 'gz')
- checks: float32 [4, 64], replicated
The draws below stay inside these ranges and needn't reach their ends.
All inputs are finite; a program needn't handle non-finite values.
Results may differ from the reference program's by a relative error of at most 0.0029.
Values may be sent and summed in bfloat16 or wider, within the bound.
No kernel may reach another device: no remote copies, remote signals or barrier semaphores. Data moves between devices by JAX's collectives and lax.ppermute only.
A program may use at most 128 MiB of HBM per device.

```python
import math
import jax
import jax.numpy as jnp
from jax import lax

D = 4096
FF = 8192
BLOCK = 128
SNAPS = 4
LAYERS = 4
NBLK = 64


def touch_ends(drawn, rng, low, high):
    dims = drawn.shape
    place = [jax.random.randint(jax.random.fold_in(rng, axis), (), 0, dims[axis]) for axis in range(len(dims))]
    drawn = drawn.at[tuple(place)].set(low)
    longest = dims.index(max(dims))
    place[longest] = (place[longest] + 1) % dims[longest]
    return drawn.at[tuple(place)].set(high)


def steps_of(rng, extent, cuts, low, top_value):
    gain = 1.0
    for position, parts in cuts:
        steps = jax.random.uniform(jax.random.fold_in(jax.random.fold_in(rng, 6), position), (parts,), jnp.float32, low / len(cuts), top_value / len(cuts))
        gain = gain * jnp.repeat(jnp.exp(steps), extent[position] // parts).reshape((-1,) + (1,) * (len(extent) - 1 - position))
    return gain


def normal_values(own_key, shape, scale, reach, cuts=(), kind=jnp.bfloat16):
    result = jax.random.normal(own_key, shape, jnp.float32) * scale
    if len(cuts) > 0:
        result = steps_of(own_key, shape, cuts, -0.22, 0.18) * result
    return jnp.clip(result, min=-reach, max=reach).astype(kind)


def setup_inputs(seed: int = 0) -> dict:
    streams_of = jax.random.split(jax.random.key(seed), 5)
    snapshots = normal_values(streams_of[0], (SNAPS, LAYERS, D, FF), 1.0, 6.0, ((1, 4), (2, 8), (3, 4)), jnp.float32)
    steps = touch_ends(jax.random.randint(streams_of[1], (SNAPS,), 0, 4000), jax.random.fold_in(streams_of[1], 1), 0, 3999).astype(jnp.int32)
    mask = touch_ends((jax.random.randint(streams_of[2], (LAYERS, NBLK), 0, 4) < 3).astype(jnp.int32), jax.random.fold_in(streams_of[2], 1), 0, 1)
    probe = normal_values(streams_of[3], (D,), 1.0, 6.0, (), jnp.float32)
    return {"snapshots": snapshots, "steps": steps, "mask": mask, "probe": probe}


decay_span = 1000.0

def blend_coef(steps):
    expo = jnp.exp(steps.astype(jnp.float32) / decay_span)
    return expo / jnp.sum(expo)

def block_checks(weights, probe_rows):
    per_col = jnp.einsum('d,ldc->lc', probe_rows, weights, preferred_element_type=jnp.float32, precision=lax.Precision.HIGHEST)
    layer_count = per_col.shape[0]
    grouped = per_col.reshape(layer_count, per_col.shape[1] // BLOCK, BLOCK)
    return lax.optimization_barrier(jnp.sum(grouped, axis=2)) / math.sqrt(D * BLOCK)

def reference(snapshots, steps, mask, probe):
    coef = blend_coef(steps)

    def one_layer(index):
        layer = lax.dynamic_index_in_dim(snapshots, index, 1, keepdims=False)
        acc = coef[0] * layer[0]
        for k in range(1, SNAPS):
            acc = acc + coef[k] * layer[k]
        row_mask = lax.dynamic_index_in_dim(mask, index, 0, keepdims=False)
        wide_mask = jnp.repeat(row_mask.astype(jnp.float32), BLOCK)
        weight_layer = (acc * wide_mask[None, :]).astype(jnp.bfloat16)
        return (weight_layer, block_checks(weight_layer[None], probe)[0])
    weights, checks = lax.map(one_layer, jnp.arange(LAYERS, dtype=jnp.int32))
    return (weights, checks)
```

```python
import functools
import math

import jax
import jax.numpy as jnp
from jax import lax
from jax.experimental import pallas as pl
from jax.experimental.pallas import tpu as pltpu
from jax.sharding import PartitionSpec as P

BLOCK = 128
DECAY_SPAN = 1000.0
ORDER = (2, 1, 3, 0)
ROWS_PER_STEP = 32
AXES = ("gx", "gy", "gz")


def blend_step(shift, first, last, steps, mask, x_ref, p_ref, part_in, w_ref, part_out, pcol, acc):
    i = pl.program_id(0)
    n = pl.num_programs(0)
    rs = x_ref.shape[2]
    nblk = x_ref.shape[3] // BLOCK
    gy = lax.axis_index("gy")
    gz = lax.axis_index("gz")
    gx = lax.axis_index("gx")
    rows = pcol.shape[0]

    @pl.when(i == 0)
    def _():
        row = gx * 4 + lax.rem(gz + shift, 4)
        pcol[...] = jnp.broadcast_to(p_ref[pl.ds(row, 1), :], (rows, BLOCK)).T
        if first:
            acc[...] = jnp.zeros_like(acc)
        else:
            acc[...] = part_in[...]

    expo = [
        jnp.exp(jnp.full((8, BLOCK), steps[k].astype(jnp.float32), jnp.float32) / DECAY_SPAN)
        for k in range(4)
    ]
    total = ((expo[0] + expo[1]) + expo[2]) + expo[3]
    coef = [jnp.broadcast_to((e / total)[None], (rs // 8, 8, BLOCK)).reshape(rs, BLOCK) for e in expo]
    probe = pcol[pl.ds(pl.multiple_of(i * rs, rs), rs), :]
    for b in range(nblk):
        cols = slice(b * BLOCK, (b + 1) * BLOCK)
        out = coef[0] * x_ref[0, 0, :, cols]
        for k in range(1, 4):
            out = out + coef[k] * x_ref[k, 0, :, cols]
        on = mask[gz, gy * nblk + b].astype(jnp.float32)
        w = (out * on).astype(jnp.bfloat16)
        w_ref[:, cols] = w
        term = probe * w.astype(jnp.float32)
        acc[b * 8 : (b + 1) * 8, :] += jnp.sum(term.reshape(rs // 8, 8, BLOCK), axis=0)

    @pl.when(i == n - 1)
    def _():
        if last:
            pcol[...] = jnp.zeros_like(pcol)
            lanes = jnp.sum(acc[...].reshape(nblk, 8, BLOCK), axis=1)
            pcol[pl.ds(pl.multiple_of(gy * nblk, nblk), nblk), :] = lanes
            mine = jnp.sum(pcol[...].T, axis=0, keepdims=True)
            part_out[...] = jnp.broadcast_to(mine, part_out.shape)
        else:
            part_out[...] = acc[...]


def blend(index, snapshots, steps, mask, probe, part):
    shift = ORDER[index]
    first, last = index == 0, index == len(ORDER) - 1
    snaps, _, rows, cols = snapshots.shape
    sub = rows // 4
    grid = sub // ROWS_PER_STEP

    def rowblock(i):
        return lax.rem(lax.axis_index("gz") + shift, 4) * grid + i

    whole = lambda i: (0, 0)
    part_shape = (128, BLOCK)
    ins = [
        pl.BlockSpec(memory_space=pltpu.SMEM),
        pl.BlockSpec(memory_space=pltpu.SMEM),
        pl.BlockSpec((snaps, 1, ROWS_PER_STEP, cols), lambda i: (0, 0, rowblock(i), 0)),
        pl.BlockSpec((32, BLOCK), whole),
    ]
    args = [steps, mask, snapshots, probe]
    if first:
        body = lambda st, mk, x, p, w, po, pc, ac: blend_step(shift, True, last, st, mk, x, p, None, w, po, pc, ac)
    else:
        body = functools.partial(blend_step, shift, False, last)
        ins.append(pl.BlockSpec(part_shape, whole))
        args.append(part)
    return pl.pallas_call(
        body,
        grid=(grid,),
        in_specs=ins,
        out_specs=[
            pl.BlockSpec((ROWS_PER_STEP, cols), lambda i: (i, 0)),
            pl.BlockSpec(part_shape, whole),
        ],
        out_shape=[
            jax.ShapeDtypeStruct((sub, cols), jnp.bfloat16),
            jax.ShapeDtypeStruct(part_shape, jnp.float32),
        ],
        scratch_shapes=[pltpu.VMEM((sub, BLOCK), jnp.float32), pltpu.VMEM((128, BLOCK), jnp.float32)],
        cost_estimate=pl.CostEstimate(
            flops=12 * sub * cols, bytes_accessed=snaps * sub * cols * 4 + sub * cols * 2, transcendentals=0
        ),
        name=f"blend{index}",
    )(*args)


def finish_kernel(got0, got1, got2, got3, parts, out, checks, sems):
    gy = lax.axis_index("gy")
    copies = []
    for j, got in enumerate((got0, got1, got2, got3)):
        slot = lax.rem(gy + 4 - ORDER[j], 4)
        copy = pltpu.make_async_copy(got, out.at[slot], sems.at[j])
        copy.start()
        copies.append(copy)
    t = jnp.sum(parts[...].reshape(16, 8, BLOCK), axis=0)
    checks[...] = (t[0:4] + t[4:8])[:, 0:64] / math.sqrt(4096 * BLOCK)
    for copy in copies:
        copy.wait()


def finish(got, parts):
    sub, cols = got[0].shape
    vmem = pl.BlockSpec(memory_space=pltpu.VMEM)
    return pl.pallas_call(
        finish_kernel,
        in_specs=[vmem] * 5,
        out_specs=[pl.BlockSpec(memory_space=pl.ANY), vmem],
        out_shape=[
            jax.ShapeDtypeStruct((4, sub, cols), jnp.bfloat16),
            jax.ShapeDtypeStruct((4, 64), jnp.float32),
        ],
        scratch_shapes=[pltpu.SemaphoreType.DMA((4,))],
        name="finish",
    )(*got, parts)


def route(shift):
    pairs = []
    for gx in range(8):
        for gy in range(4):
            for gz in range(4):
                pairs.append((gx * 16 + gy * 4 + gz, gx * 16 + ((gz + shift) % 4) * 4 + gy))
    return pairs


def local(snapshots, steps, mask, probe):
    probe = probe.reshape(32, BLOCK)
    part = None
    got = []
    for index, shift in enumerate(ORDER):
        w, part = blend(index, snapshots, steps, mask, probe, part)
        got.append(lax.ppermute(w, AXES, route(shift)))
    parts = lax.all_to_all(part, AXES, 0, 0, tiled=True)
    return tuple(finish(got, parts))


def solution(mesh):
    return jax.shard_map(
        local,
        mesh=mesh,
        in_specs=(P(None, "gz", "gx", "gy"), P(), P(), P()),
        out_specs=(P(None, ("gx", "gy"), "gz"), P()),
        check_vma=False,
    )
```

```python
import functools
import math

import jax
import jax.numpy as jnp
from jax import lax
from jax.experimental import pallas as pl
from jax.experimental.pallas import tpu as pltpu
from jax.sharding import PartitionSpec as P

BLOCK = 128
DECAY_SPAN = 1000.0
GROUPS = ((0, 1), (2, 3))
CHUNK = 32
AXES = ("gx", "gy", "gz")
STAGES = (
    ((1, 3, 0, 2), (2, 0, 3, 1), (1, 3, 0, 2), (2, 0, 3, 1)),
    ((2, 0, 3, 1), (1, 3, 0, 2), (2, 0, 3, 1), (1, 3, 0, 2)),
    ((3, 1, 2, 0), (0, 2, 1, 3), (3, 1, 2, 0), (0, 2, 1, 3)),
    ((0, 2, 1, 3), (3, 1, 2, 0), (0, 2, 1, 3), (3, 1, 2, 0)),
)


def lookup(table, i, j):
    packed = sum(table[m][n] << (2 * (4 * m + n)) for m in range(4) for n in range(4))
    packed = packed - (1 << 32) if packed >= 1 << 31 else packed
    return jnp.bitwise_and(lax.shift_right_logical(jnp.int32(packed), (4 * i + j) * 2), 3)


def sent_to(stage, gy, gz):
    return lookup(STAGES[stage], gy, gz)


def layer_from(stage, gy, gz):
    inverse = [[row.index(r) for r in range(4)] for row in STAGES[stage]]
    return lookup(inverse, gz, gy)


def blend_kernel(stages, first, last, *refs):
    steps_hbm, mask_hbm, probe_hbm, x_hbm = refs[:4]
    refs = refs[4:]
    if not first:
        part_in, refs = refs[0], refs[1:]
    w_refs, refs = refs[: len(stages)], refs[len(stages) :]
    part_out, xbuf, steps, mask, p_ref, pcol, acc, small, sems = refs
    nblk = x_hbm.shape[3] // BLOCK
    sub = x_hbm.shape[2] // 4
    per = sub // CHUNK
    gx, gy, gz = (lax.axis_index(a) for a in AXES)
    quarter = [sent_to(s, gy, gz) for s in stages]

    tables = [
        pltpu.make_async_copy(src, dst, small.at[i])
        for i, (src, dst) in enumerate(((steps_hbm, steps), (probe_hbm, p_ref), (mask_hbm, mask)))
    ]

    def fetch(j, c):
        row = pl.multiple_of(quarter[j] * sub + c * CHUNK, CHUNK)
        here = pl.ds(pl.multiple_of(c * CHUNK, CHUNK), CHUNK)
        return pltpu.make_async_copy(
            x_hbm.at[:, 0, pl.ds(row, CHUNK), :], xbuf.at[j, :, here, :], sems.at[j, c]
        )

    for t in tables:
        t.start()
    for j in range(len(stages)):
        for c in range(per):
            fetch(j, c).start()
    for t in tables:
        t.wait()

    if first:
        acc[...] = jnp.zeros_like(acc)
    else:
        acc[...] = part_in[...]
    expo = [
        jnp.exp(jnp.full((8, BLOCK), steps[k].astype(jnp.float32), jnp.float32) / DECAY_SPAN)
        for k in range(4)
    ]
    total = ((expo[0] + expo[1]) + expo[2]) + expo[3]
    coef = [e / total for e in expo]
    wide = [jnp.broadcast_to(c[None], (CHUNK // 8, 8, BLOCK)).reshape(CHUNK, BLOCK) for c in coef]

    for j in range(len(stages)):
        pcol[j] = jnp.broadcast_to(p_ref[pl.ds(gx * 4 + quarter[j], 1), :], (sub, BLOCK)).T

    for j in range(len(stages)):

        def chunk(c, carry):
            fetch(j, c).wait()
            rows = pl.ds(pl.multiple_of(c * CHUNK, CHUNK), CHUNK)
            probe = pcol[j, rows, :]
            for b in range(nblk):
                cols = slice(b * BLOCK, (b + 1) * BLOCK)
                out = wide[0] * xbuf[j, 0, rows, cols]
                for k in range(1, 4):
                    out = out + wide[k] * xbuf[j, k, rows, cols]
                on = mask[gz, gy * nblk + b].astype(jnp.float32)
                w = (out * on).astype(jnp.bfloat16)
                w_refs[j][rows, cols] = w
                term = probe * w.astype(jnp.float32)
                acc[b * 8 : (b + 1) * 8, :] += jnp.sum(term.reshape(CHUNK // 8, 8, BLOCK), axis=0)
            return carry

        lax.fori_loop(0, per, chunk, 0)

    if last:
        lanes = jnp.sum(acc[...].reshape(nblk, 8, BLOCK), axis=1)
        acc[...] = jnp.zeros_like(acc)
        acc[pl.ds(pl.multiple_of(gy * nblk, nblk), nblk), :] = lanes
        mine = jnp.sum(acc[...].T, axis=0, keepdims=True)
        part_out[...] = jnp.broadcast_to(mine, part_out.shape)
    else:
        part_out[...] = acc[...]


def blend(index, snapshots, steps, mask, probe, part):
    stages = GROUPS[index]
    first, last = index == 0, index == len(GROUPS) - 1
    snaps, _, rows, cols = snapshots.shape
    sub = rows // 4
    n = len(stages)
    hbm, vmem = pl.BlockSpec(memory_space=pltpu.HBM), pl.BlockSpec(memory_space=pltpu.VMEM)
    args = [pltpu.with_memory_space_constraint(a, pltpu.HBM) for a in (steps, mask, probe, snapshots)]
    ins = [hbm] * 4
    if not first:
        ins.append(vmem)
        args.append(pltpu.with_memory_space_constraint(part, pltpu.VMEM))
    return pl.pallas_call(
        functools.partial(blend_kernel, stages, first, last),
        in_specs=ins,
        out_specs=[vmem] * (n + 1),
        out_shape=[pltpu.VMEM((sub, cols), jnp.bfloat16)] * n + [pltpu.VMEM((128, BLOCK), jnp.float32)],
        scratch_shapes=[
            pltpu.VMEM((n, snaps, sub, cols), jnp.float32),
            pltpu.SMEM(steps.shape, jnp.int32),
            pltpu.SMEM(mask.shape, jnp.int32),
            pltpu.VMEM(probe.shape, jnp.float32),
            pltpu.VMEM((n, sub, BLOCK), jnp.float32),
            pltpu.VMEM((128, BLOCK), jnp.float32),
            pltpu.SemaphoreType.DMA((3,)),
            pltpu.SemaphoreType.DMA((n, sub // CHUNK)),
        ],
        cost_estimate=pl.CostEstimate(
            flops=12 * n * sub * cols, bytes_accessed=n * sub * cols * (snaps * 4 + 2), transcendentals=0
        ),
        compiler_params=pltpu.CompilerParams(vmem_limit_bytes=54 << 20),
        name=f"blend{index}",
    )(*args)


def totals_kernel(parts, checks):
    t = jnp.sum(parts[...].reshape(16, 8, BLOCK), axis=0)
    checks[...] = (t[0:4] + t[4:8])[:, 0:64] / math.sqrt(4096 * BLOCK)


def totals(parts):
    return pl.pallas_call(
        totals_kernel,
        out_shape=jax.ShapeDtypeStruct((4, 64), jnp.float32),
        compiler_params=pltpu.CompilerParams(vmem_limit_bytes=54 << 20),
        name="totals",
    )(parts)


def finish_kernel(order, *refs):
    got, (out, sems) = refs[:4], refs[4:]
    gy, gz = lax.axis_index("gy"), lax.axis_index("gz")
    copies = []
    for j in range(4):
        slot = layer_from(order[j], gy, gz)
        copy = pltpu.make_async_copy(got[j], out.at[slot], sems.at[j])
        copy.start()
        copies.append(copy)
    for copy in copies:
        copy.wait()


def finish(order, got):
    sub, cols = got[0].shape
    vmem = pl.BlockSpec(memory_space=pltpu.VMEM)
    got = [pltpu.with_memory_space_constraint(g, pltpu.VMEM) for g in got]
    return pl.pallas_call(
        functools.partial(finish_kernel, order),
        in_specs=[vmem] * 4,
        out_specs=pl.BlockSpec(memory_space=pltpu.HBM),
        out_shape=jax.ShapeDtypeStruct((4, sub, cols), jnp.bfloat16),
        scratch_shapes=[pltpu.SemaphoreType.DMA((4,))],
        compiler_params=pltpu.CompilerParams(vmem_limit_bytes=54 << 20),
        name="finish",
    )(*got)


def route(shift):
    pairs = []
    for gx in range(8):
        for gy in range(4):
            for gz in range(4):
                pairs.append((gx * 16 + gy * 4 + gz, gx * 16 + STAGES[shift][gy][gz] * 4 + gy))
    return pairs


def local(snapshots, steps, mask, probe):
    probe = probe.reshape(32, BLOCK)
    part = None
    got = []
    order = sum(GROUPS, ())
    for index, shifts in enumerate(GROUPS):
        *ws, part = blend(index, snapshots, steps, mask, probe, part)
        got += [lax.ppermute(w, AXES, route(s)) for w, s in zip(ws, shifts)]
    parts = lax.all_to_all(part, AXES, 0, 0, tiled=True)
    return finish(order, got), totals(parts)


def solution(mesh):
    return jax.shard_map(
        local,
        mesh=mesh,
        in_specs=(P(None, "gz", "gx", "gy"), P(), P(), P()),
        out_specs=(P(None, ("gx", "gy"), "gz"), P()),
        check_vma=False,
    )
```

```python
import functools
import math

import jax
import jax.numpy as jnp
from jax import lax
from jax.experimental import pallas as pl
from jax.experimental.pallas import tpu as pltpu
from jax.sharding import Mesh
from jax.sharding import PartitionSpec as P


BLOCK = 128
DECAY_SPAN = 1000.0
GROUPS = ((0, 1), (2, 3))
CHUNK = 32
AXES = ("ylo", "z", "gy", "yhi", "core")
STAGES = (
    ((1, 3, 0, 2), (2, 0, 3, 1), (1, 3, 0, 2), (2, 0, 3, 1)),
    ((2, 0, 3, 1), (1, 3, 0, 2), (2, 0, 3, 1), (1, 3, 0, 2)),
    ((3, 1, 2, 0), (0, 2, 1, 3), (3, 1, 2, 0), (0, 2, 1, 3)),
    ((0, 2, 1, 3), (3, 1, 2, 0), (0, 2, 1, 3), (3, 1, 2, 0)),
)


def lookup(table, i, j):
    packed = sum(table[m][n] << (2 * (4 * m + n)) for m in range(4) for n in range(4))
    packed = packed - (1 << 32) if packed >= 1 << 31 else packed
    return jnp.bitwise_and(lax.shift_right_logical(jnp.int32(packed), (4 * i + j) * 2), 3)


def place():
    ylo, z, gy, yhi, core = (lax.axis_index(a) for a in AXES)
    return ylo * 4 + z, gy, yhi * 2 + core


def sent_to(stage, gy, gz):
    return lookup(STAGES[stage], gy, gz)


def layer_from(stage, gy, gz):
    inverse = [[row.index(r) for r in range(4)] for row in STAGES[stage]]
    return lookup(inverse, gz, gy)


def blend_kernel(stages, first, last, *refs):
    steps_hbm, mask_hbm, probe_hbm, x_hbm = refs[:4]
    refs = refs[4:]
    if not first:
        part_in, refs = refs[0], refs[1:]
    w_refs, refs = refs[: len(stages)], refs[len(stages) :]
    part_out, xbuf, steps, mask, p_ref, pcol, acc, small, sems = refs
    nblk = x_hbm.shape[3] // BLOCK
    sub = x_hbm.shape[2] // 4
    per = sub // CHUNK
    gx, gy, gz = place()
    quarter = [sent_to(s, gy, gz) for s in stages]

    tables = [
        pltpu.make_async_copy(src, dst, small.at[i])
        for i, (src, dst) in enumerate(((steps_hbm, steps), (probe_hbm, p_ref), (mask_hbm, mask)))
    ]

    def fetch(j, c):
        row = pl.multiple_of(quarter[j] * sub + c * CHUNK, CHUNK)
        here = pl.ds(pl.multiple_of(c * CHUNK, CHUNK), CHUNK)
        return pltpu.make_async_copy(
            x_hbm.at[:, 0, pl.ds(row, CHUNK), :], xbuf.at[j, :, here, :], sems.at[j, c]
        )

    for t in tables:
        t.start()
    for j in range(len(stages)):
        for c in range(per):
            fetch(j, c).start()
    for t in tables:
        t.wait()

    if first:
        acc[...] = jnp.zeros_like(acc)
    else:
        acc[...] = part_in[...]
    expo = [
        jnp.exp(jnp.full((8, BLOCK), steps[k].astype(jnp.float32), jnp.float32) / DECAY_SPAN)
        for k in range(4)
    ]
    total = ((expo[0] + expo[1]) + expo[2]) + expo[3]
    coef = [e / total for e in expo]
    wide = [jnp.broadcast_to(c[None], (CHUNK // 8, 8, BLOCK)).reshape(CHUNK, BLOCK) for c in coef]

    for j in range(len(stages)):
        pcol[j] = jnp.broadcast_to(p_ref[pl.ds(gx * 4 + quarter[j], 1), :], (sub, BLOCK)).T

    for j in range(len(stages)):

        def chunk(c, carry):
            fetch(j, c).wait()
            rows = pl.ds(pl.multiple_of(c * CHUNK, CHUNK), CHUNK)
            probe = pcol[j, rows, :]
            for b in range(nblk):
                cols = slice(b * BLOCK, (b + 1) * BLOCK)
                out = wide[0] * xbuf[j, 0, rows, cols]
                for k in range(1, 4):
                    out = out + wide[k] * xbuf[j, k, rows, cols]
                on = mask[gz, gy * nblk + b].astype(jnp.float32)
                w = (out * on).astype(jnp.bfloat16)
                w_refs[j][rows, cols] = w
                term = probe * w.astype(jnp.float32)
                acc[b * 8 : (b + 1) * 8, :] += jnp.sum(term.reshape(CHUNK // 8, 8, BLOCK), axis=0)
            return carry

        lax.fori_loop(0, per, chunk, 0)

    if last:
        lanes = jnp.sum(acc[...].reshape(nblk, 8, BLOCK), axis=1)
        acc[...] = jnp.zeros_like(acc)
        spot = lax.axis_index("yhi") * 4 + gy
        acc[pl.ds(pl.multiple_of(spot * nblk, nblk), nblk), :] = lanes
        mine = jnp.sum(acc[...].T, axis=0, keepdims=True)
        part_out[...] = jnp.broadcast_to(mine, part_out.shape)
    else:
        part_out[...] = acc[...]


def blend(index, snapshots, steps, mask, probe, part):
    stages = GROUPS[index]
    first, last = index == 0, index == len(GROUPS) - 1
    snaps, _, rows, cols = snapshots.shape
    sub = rows // 4
    n = len(stages)
    hbm, vmem = pl.BlockSpec(memory_space=pltpu.HBM), pl.BlockSpec(memory_space=pltpu.VMEM)
    args = [pltpu.with_memory_space_constraint(a, pltpu.HBM) for a in (steps, mask, probe, snapshots)]
    ins = [hbm] * 4
    if not first:
        ins.append(vmem)
        args.append(pltpu.with_memory_space_constraint(part, pltpu.VMEM))
    return pl.pallas_call(
        functools.partial(blend_kernel, stages, first, last),
        in_specs=ins,
        out_specs=[vmem] * (n + 1),
        out_shape=[pltpu.VMEM((sub, cols), jnp.bfloat16)] * n + [pltpu.VMEM((128, BLOCK), jnp.float32)],
        scratch_shapes=[
            pltpu.VMEM((n, snaps, sub, cols), jnp.float32),
            pltpu.SMEM(steps.shape, jnp.int32),
            pltpu.SMEM(mask.shape, jnp.int32),
            pltpu.VMEM(probe.shape, jnp.float32),
            pltpu.VMEM((n, sub, BLOCK), jnp.float32),
            pltpu.VMEM((128, BLOCK), jnp.float32),
            pltpu.SemaphoreType.DMA((3,)),
            pltpu.SemaphoreType.DMA((n, sub // CHUNK)),
        ],
        cost_estimate=pl.CostEstimate(
            flops=12 * n * sub * cols, bytes_accessed=n * sub * cols * (snaps * 4 + 2), transcendentals=0
        ),
        compiler_params=pltpu.CompilerParams(vmem_limit_bytes=49 << 20),
    )(*args)


def totals_kernel(parts, checks):
    half = checks.shape[1]
    t = jnp.sum(parts[...].reshape(16, 8, BLOCK), axis=0)
    t = ((t[0:2] + t[2:4]) + (t[4:6] + t[6:8])) / math.sqrt(4096 * BLOCK)
    checks[0:2] = t[:, :half]
    checks[2:4] = t[:, half:]


def totals(parts):
    return pl.pallas_call(
        totals_kernel,
        out_shape=jax.ShapeDtypeStruct((4, 64), jnp.float32),
        compiler_params=pltpu.CompilerParams(vmem_limit_bytes=4 << 20),
        name="totals",
    )(parts)


def finish_kernel(order, *refs):
    got, (out, sems) = refs[:4], refs[4:]
    _, gy, gz = place()
    copies = []
    for j in range(4):
        slot = layer_from(order[j], gy, gz)
        copy = pltpu.make_async_copy(got[j], out.at[slot], sems.at[j])
        copy.start()
        copies.append(copy)
    for copy in copies:
        copy.wait()


def finish(order, got):
    sub, cols = got[0].shape
    vmem = pl.BlockSpec(memory_space=pltpu.VMEM)
    got = [pltpu.with_memory_space_constraint(g, pltpu.VMEM) for g in got]
    return pl.pallas_call(
        functools.partial(finish_kernel, order),
        in_specs=[vmem] * 4,
        out_specs=pl.BlockSpec(memory_space=pltpu.HBM),
        out_shape=jax.ShapeDtypeStruct((4, sub, cols), jnp.bfloat16),
        scratch_shapes=[pltpu.SemaphoreType.DMA((4,))],
        compiler_params=pltpu.CompilerParams(vmem_limit_bytes=4 << 20),
        name="finish",
    )(*got)


def route(shift):
    pairs = []
    for gx in range(8):
        for gy in range(4):
            for gz in range(4):
                pairs.append((gx * 16 + gy * 4 + gz, gx * 16 + STAGES[shift][gy][gz] * 4 + gy))
    return pairs


def exchange(ws, stages):
    moved = []
    for w, s in zip(ws, stages):
        moved.append(lax.ppermute(w, AXES, route(s)))
    return moved


def gather_checks(part):
    return totals(lax.all_to_all(part, AXES, 0, 0, tiled=True))


def consolidate(snapshots, steps, mask, probe):
    probe = probe.reshape(32, BLOCK)
    part = None
    got = []
    for index, stages in enumerate(GROUPS):
        *ws, part = blend(index, snapshots, steps, mask, probe, part)
        got += exchange(ws, stages)
    checks = gather_checks(part)
    return finish(sum(GROUPS, ()), got), checks


def solution(mesh):
    split = Mesh(mesh.devices.reshape(2, 4, 4, 2, 2), AXES)
    return jax.shard_map(
        consolidate,
        mesh=split,
        in_specs=(P(None, ("yhi", "core"), ("ylo", "z"), "gy"), P(), P(), P()),
        out_specs=(P(None, ("ylo", "z", "gy"), ("yhi", "core")), P()),
        check_vma=False,
    )
```

```python
import functools
import math

import jax
import jax.numpy as jnp
from jax import lax
from jax.experimental import pallas as pl
from jax.experimental.pallas import tpu as pltpu
from jax.sharding import Mesh
from jax.sharding import PartitionSpec as P


BLOCK = 128
DECAY_SPAN = 1000.0
GROUPS = ((0, 1), (2, 3))
CHUNK = 32
AXES = ("ylo", "z", "gy", "yhi", "core")
STAGES = (
    ((1, 3, 2, 0), (2, 0, 3, 1), (1, 3, 0, 2), (0, 2, 3, 1)),
    ((2, 0, 1, 3), (1, 3, 0, 2), (2, 0, 1, 3), (3, 1, 2, 0)),
    ((3, 1, 0, 2), (0, 2, 1, 3), (3, 1, 2, 0), (2, 0, 1, 3)),
    ((0, 2, 3, 1), (3, 1, 2, 0), (0, 2, 3, 1), (1, 3, 0, 2)),
)


def lookup(table, i, j):
    packed = sum(table[m][n] << (2 * (4 * m + n)) for m in range(4) for n in range(4))
    packed = packed - (1 << 32) if packed >= 1 << 31 else packed
    return jnp.bitwise_and(lax.shift_right_logical(jnp.int32(packed), (4 * i + j) * 2), 3)


def place():
    ylo, z, gy, yhi, core = (lax.axis_index(a) for a in AXES)
    return ylo * 4 + z, gy, yhi * 2 + core


def sent_to(stage, gy, gz):
    return lookup(STAGES[stage], gy, gz)


def layer_from(stage, gy, gz):
    inverse = [[row.index(r) for r in range(4)] for row in STAGES[stage]]
    return lookup(inverse, gz, gy)


def blend_kernel(stages, first, last, *refs):
    steps_hbm, mask_hbm, probe_hbm, x_hbm = refs[:4]
    refs = refs[4:]
    if not first:
        part_in, refs = refs[0], refs[1:]
    w_refs, refs = refs[: len(stages)], refs[len(stages) :]
    part_out, xbuf, steps, mask, p_ref, pcol, acc, small, sems = refs
    nblk = x_hbm.shape[3] // BLOCK
    sub = x_hbm.shape[2] // 4
    per = sub // CHUNK
    gx, gy, gz = place()
    quarter = [sent_to(s, gy, gz) for s in stages]

    tables = [
        pltpu.make_async_copy(src, dst, small.at[i])
        for i, (src, dst) in enumerate(((steps_hbm, steps), (probe_hbm, p_ref), (mask_hbm, mask)))
    ]

    def fetch(j, c):
        row = pl.multiple_of(quarter[j] * sub + c * CHUNK, CHUNK)
        here = pl.ds(pl.multiple_of(c * CHUNK, CHUNK), CHUNK)
        return pltpu.make_async_copy(
            x_hbm.at[:, 0, pl.ds(row, CHUNK), :], xbuf.at[j, :, here, :], sems.at[j, c]
        )

    for t in tables:
        t.start()
    for j in range(len(stages)):
        for c in range(per):
            fetch(j, c).start()
    for t in tables:
        t.wait()

    if first:
        acc[...] = jnp.zeros_like(acc)
    else:
        acc[...] = part_in[...]
    expo = [
        jnp.exp(jnp.full((8, BLOCK), steps[k].astype(jnp.float32), jnp.float32) / DECAY_SPAN)
        for k in range(4)
    ]
    total = ((expo[0] + expo[1]) + expo[2]) + expo[3]
    coef = [e / total for e in expo]
    wide = [jnp.broadcast_to(c[None], (CHUNK // 8, 8, BLOCK)).reshape(CHUNK, BLOCK) for c in coef]

    for j in range(len(stages)):
        pcol[j] = jnp.broadcast_to(p_ref[pl.ds(gx * 4 + quarter[j], 1), :], (sub, BLOCK)).T

    for j in range(len(stages)):

        def chunk(c, carry):
            fetch(j, c).wait()
            rows = pl.ds(pl.multiple_of(c * CHUNK, CHUNK), CHUNK)
            probe = pcol[j, rows, :]
            for b in range(nblk):
                cols = slice(b * BLOCK, (b + 1) * BLOCK)
                out = wide[0] * xbuf[j, 0, rows, cols]
                for k in range(1, 4):
                    out = out + wide[k] * xbuf[j, k, rows, cols]
                on = mask[gz, gy * nblk + b].astype(jnp.float32)
                w = (out * on).astype(jnp.bfloat16)
                w_refs[j][rows, cols] = w
                term = probe * w.astype(jnp.float32)
                acc[b * 8 : (b + 1) * 8, :] += jnp.sum(term.reshape(CHUNK // 8, 8, BLOCK), axis=0)
            return carry

        lax.fori_loop(0, per, chunk, 0)

    if last:
        lanes = jnp.sum(acc[...].reshape(nblk, 8, BLOCK), axis=1)
        acc[...] = jnp.zeros_like(acc)
        spot = lax.axis_index("yhi") * 4 + gy
        acc[pl.ds(pl.multiple_of(spot * nblk, nblk), nblk), :] = lanes
        mine = jnp.sum(acc[...].T, axis=0, keepdims=True)
        part_out[...] = jnp.broadcast_to(mine, part_out.shape)
    else:
        part_out[...] = acc[...]


def blend(index, snapshots, steps, mask, probe, part):
    stages = GROUPS[index]
    first, last = index == 0, index == len(GROUPS) - 1
    snaps, _, rows, cols = snapshots.shape
    sub = rows // 4
    n = len(stages)
    hbm, vmem = pl.BlockSpec(memory_space=pltpu.HBM), pl.BlockSpec(memory_space=pltpu.VMEM)
    args = [pltpu.with_memory_space_constraint(a, pltpu.HBM) for a in (steps, mask, probe, snapshots)]
    ins = [hbm] * 4
    if not first:
        ins.append(vmem)
        args.append(pltpu.with_memory_space_constraint(part, pltpu.VMEM))
    return pl.pallas_call(
        functools.partial(blend_kernel, stages, first, last),
        in_specs=ins,
        out_specs=[vmem] * (n + 1),
        out_shape=[pltpu.VMEM((sub, cols), jnp.bfloat16)] * n + [pltpu.VMEM((128, BLOCK), jnp.float32)],
        scratch_shapes=[
            pltpu.VMEM((n, snaps, sub, cols), jnp.float32),
            pltpu.SMEM(steps.shape, jnp.int32),
            pltpu.SMEM(mask.shape, jnp.int32),
            pltpu.VMEM(probe.shape, jnp.float32),
            pltpu.VMEM((n, sub, BLOCK), jnp.float32),
            pltpu.VMEM((128, BLOCK), jnp.float32),
            pltpu.SemaphoreType.DMA((3,)),
            pltpu.SemaphoreType.DMA((n, sub // CHUNK)),
        ],
        cost_estimate=pl.CostEstimate(
            flops=12 * n * sub * cols, bytes_accessed=n * sub * cols * (snaps * 4 + 2), transcendentals=0
        ),
        compiler_params=pltpu.CompilerParams(vmem_limit_bytes=49 << 20),
    )(*args)


def totals_kernel(parts, checks):
    half = checks.shape[1]
    t = jnp.sum(parts[...].reshape(16, 8, BLOCK), axis=0)
    t = ((t[0:2] + t[2:4]) + (t[4:6] + t[6:8])) / math.sqrt(4096 * BLOCK)
    checks[0:2] = t[:, :half]
    checks[2:4] = t[:, half:]


def totals(parts):
    return pl.pallas_call(
        totals_kernel,
        out_shape=jax.ShapeDtypeStruct((4, 64), jnp.float32),
        compiler_params=pltpu.CompilerParams(vmem_limit_bytes=4 << 20),
        name="totals",
    )(parts)


def finish_kernel(order, *refs):
    got, (out, sems) = refs[:4], refs[4:]
    _, gy, gz = place()
    copies = []
    for j in range(4):
        slot = layer_from(order[j], gy, gz)
        copy = pltpu.make_async_copy(got[j], out.at[slot], sems.at[j])
        copy.start()
        copies.append(copy)
    for copy in copies:
        copy.wait()


def finish(order, got):
    sub, cols = got[0].shape
    vmem = pl.BlockSpec(memory_space=pltpu.VMEM)
    got = [pltpu.with_memory_space_constraint(g, pltpu.VMEM) for g in got]
    return pl.pallas_call(
        functools.partial(finish_kernel, order),
        in_specs=[vmem] * 4,
        out_specs=pl.BlockSpec(memory_space=pltpu.HBM),
        out_shape=jax.ShapeDtypeStruct((4, sub, cols), jnp.bfloat16),
        scratch_shapes=[pltpu.SemaphoreType.DMA((4,))],
        compiler_params=pltpu.CompilerParams(vmem_limit_bytes=4 << 20),
        name="finish",
    )(*got)


def route(shift):
    pairs = []
    for gx in range(8):
        for gy in range(4):
            for gz in range(4):
                pairs.append((gx * 16 + gy * 4 + gz, gx * 16 + STAGES[shift][gy][gz] * 4 + gy))
    return pairs


def exchange(ws, stages):
    moved = []
    for w, s in zip(ws, stages):
        moved.append(lax.ppermute(w, AXES, route(s)))
    return moved


def gather_checks(part):
    return totals(lax.all_to_all(part, AXES, 0, 0, tiled=True))


def consolidate(snapshots, steps, mask, probe):
    probe = probe.reshape(32, BLOCK)
    part = None
    got = []
    for index, stages in enumerate(GROUPS):
        *ws, part = blend(index, snapshots, steps, mask, probe, part)
        got += exchange(ws, stages)
    checks = gather_checks(part)
    return finish(sum(GROUPS, ()), got), checks


def solution(mesh):
    split = Mesh(mesh.devices.reshape(2, 4, 4, 2, 2), AXES)
    return jax.shard_map(
        consolidate,
        mesh=split,
        in_specs=(P(None, ("yhi", "core"), ("ylo", "z"), "gy"), P(), P(), P()),
        out_specs=(P(None, ("ylo", "z", "gy"), ("yhi", "core")), P()),
        check_vma=False,
    )
```
